32 devices in a mesh: dp: 2 (over core), ctx: 4 (over y, x), enc: 4 (over z).
Axes of the slice: x: 2, y: 2, z: 4, core: 2. Of those that a mesh axis runs over, the one named last changes fastest.
Arguments:
- hidden: bfloat16 [2048, 4096], P(('dp', 'ctx')), may hold values from -16 to 16
- neighbour_states: bfloat16 [128, 128, 896], P(('dp', 'ctx', 'enc')), may hold values from -16 to 16
- neighbour_owner: int32 [32, 2], P(('dp', 'ctx')), may hold values from 0 to 3, all different within a row; in each aligned block of 4 rows (0 to 3, 4 to 7, ...) at most 4 rows name the same one
- query_weight: bfloat16 [4096, 2048], P('dp', 'enc'), may hold values from -0.09375 to 0.09375
- key_weight: bfloat16 [896, 2048], P('dp', 'enc'), may hold values from -0.1875 to 0.1875
- value_weight: bfloat16 [896, 2048], P('dp', 'enc'), may hold values from -0.1875 to 0.1875
- out_weight: bfloat16 [2048, 4096], P('dp', 'enc'), may hold values from -0.5 to 0.5
- cotangent: bfloat16 [2048, 4096], P(('dp', 'ctx'), 'enc'), may hold values from -0.119628906 to 0.119628906
Outputs:
- mixed: bfloat16 [2048, 4096], P(('dp', 'ctx'), 'enc')
- grad_query_weight: float32 [4096, 2048], P('dp', 'enc')
The draws below stay inside these ranges and needn't reach their ends.
Inputs may be any that keep to these rules, and one draw needn't show every extreme that they name: `neighbour_owner`: the 2 neighbours of a span lie at different owners; within the rows of one device (4 spans, aligned blocks) no owner is named more than 4 times.
All inputs are finite; a program needn't handle non-finite values.
Results may differ from the reference program's by a relative error of at most 0.024.
Values may be sent and summed in bfloat16 or wider, within the bound.
No kernel may reach another device: no remote copies, remote signals or barrier semaphores. Data moves between devices by JAX's collectives and lax.ppermute only.
A program may use at most 64 MiB of HBM per device.

```python
import math
import jax
import jax.numpy as jnp
import numpy as np
from jax import lax

D = 4096
ENC_D = 896
HEADS = 16
HEAD_DIM = 128
SPAN = 64
NEIGHBOURS = 2
NEIGH_LEN = 128
SPANS_DEV = 4
PROJ = 2048
SLOTS = 4
SEQ_LEN = 1024
TOKENS = 2048
ALL_SPANS = 32
ALL_SLOTS = 128
N_DP = 2
N_CTX = 4
N_ENC = 4


def spread_rows(key, shape):
    base_key = jax.random.fold_in(jax.random.fold_in(key, 11), 0)
    values = jax.random.normal(base_key, shape, jnp.float32)
    return jnp.clip(values, -6.0, 6.0)


def draw_hidden(key, part):
    return spread_rows(key, (TOKENS, D)).astype(jnp.bfloat16)


def draw_neighbour_states(key, part):
    return spread_rows(jax.random.fold_in(key, 23), (ALL_SLOTS, NEIGH_LEN, ENC_D)).astype(jnp.bfloat16)


def shard_levels(rng, extent, cuts, least, top_value):
    factor_of, own = 1.0, jax.random.fold_in(rng, 6)
    for axis_at, blocks in cuts:
        draws = jnp.exp(jax.random.uniform(jax.random.fold_in(own, axis_at), (blocks,), jnp.float32, least / len(cuts), top_value / len(cuts)))
        factor_of = factor_of * jnp.repeat(draws, extent[axis_at] // blocks).reshape([-1 if axis == axis_at else 1 for axis in range(len(extent))])
    return factor_of


def routed_block(key, own, number, rows, amount, top, reach, slope):
    sequence = jax.random.permutation(key, amount)
    heavy_load, ordinary = portions_of(amount, rows * top, reach, slope, True), portions_of(amount, rows * top, reach, slope, False)
    places = jnp.arange(amount)

    def named(tallies, offset_by):
        used = int((tallies > 0).sum())
        fixed = max(1, used // 4)
        moved = fixed + (places - fixed + offset_by * (used - fixed)) % max(1, amount - fixed)
        return jnp.zeros((amount,), jnp.int32).at[sequence[jnp.where(places < fixed, places, moved)]].set(jnp.asarray(tallies, jnp.int32))

    tallies = jnp.where(number % 4 == 0, named(heavy_load, number // 4), named(ordinary, number - number // 4 - 1))
    mixed = jax.random.permutation(jax.random.fold_in(own, 3), amount)
    giver, taker = mixed[0:amount // 2 * 2:2], mixed[1:amount // 2 * 2:2]
    margin = jnp.minimum(tallies[giver] - 1, reach - tallies[taker]) // 2
    margin = jnp.where((giver == sequence[0]) | (taker == sequence[0]) | (tallies[taker] == 0), 0, jnp.maximum(margin, 0))
    moved = jax.random.randint(jax.random.fold_in(own, 4), (amount // 2,), 0, 1 << 20) % (margin + 1)
    tallies = tallies.at[giver].add(-moved).at[taker].add(moved)
    labels = jnp.searchsorted(jnp.cumsum(tallies), jnp.arange(rows * top), side="right").astype(jnp.int32)
    table = labels.reshape(top, rows).T
    table = table[jax.random.permutation(jax.random.fold_in(own, 1), rows)]
    offset_by = jax.random.randint(jax.random.fold_in(own, 2), (rows, 1), 0, top)
    return jnp.take_along_axis(table, (jnp.arange(top)[None, :] + offset_by) % top, axis=1)


def portions_of(amount, total, most, skew, full):
    weights = [(1 << 20) // math.isqrt(standing ** skew) + 1 for standing in range(1, amount + 1)]
    largest = most if full else min(most, max(-(-total // amount), total * weights[0] // sum(weights)))
    least = 1 if total - largest >= amount - 1 else 0
    counts, surplus = [largest] + [least] * (amount - 1), total - largest - least * (amount - 1)
    while surplus > 0:
        free = [i for i in range(1, amount) if counts[i] < largest] or [i for i in range(1, amount) if counts[i] < most]
        pool, left = sum([weights[i] for i in free]), surplus
        for i in free:
            extra = min(most - counts[i], max(1, left * weights[i] // pool), surplus)
            counts[i] = counts[i] + extra
            surplus = surplus - extra
    return np.array(counts)


def noise(rng, shape, deviation, limit, shards=(), kind=jnp.bfloat16):
    factor_of = shard_levels(rng, shape, shards, -0.22, 0.18) if shards else 1.0
    result = jax.random.normal(rng, shape, jnp.float32) * deviation * factor_of
    return jnp.minimum(jnp.maximum(result, -limit), limit).astype(kind)


def setup_inputs(seed: int = 0) -> dict:
    key_list = jax.random.split(jax.random.key(seed), 9)
    hidden = draw_hidden(jax.random.fold_in(key_list[8], 71), 0)
    neighbour_states = draw_neighbour_states(jax.random.fold_in(key_list[8], 71), 0)
    neighbour_owner_keys = jax.random.split(jax.random.fold_in(key_list[2], 1), ALL_SPANS // SPANS_DEV)
    neighbour_owner_turns = jax.random.permutation(jax.random.fold_in(key_list[2], 3), ALL_SPANS // SPANS_DEV)
    neighbour_owner = jax.vmap(lambda own, number: routed_block(jax.random.fold_in(key_list[2], 2), own, number, SPANS_DEV, N_ENC, NEIGHBOURS, SLOTS, 2))(neighbour_owner_keys, neighbour_owner_turns).reshape((ALL_SPANS, NEIGHBOURS))
    query_weight = noise(key_list[3], (D, PROJ), D ** -0.5, 0.09375, ((0, 2), (1, 4)))
    key_weight = noise(key_list[4], (ENC_D, PROJ), ENC_D ** -0.5, 0.1875, ((0, 2), (1, 4)))
    value_weight = noise(key_list[5], (ENC_D, PROJ), ENC_D ** -0.5, 0.1875, ((0, 2), (1, 4)))
    out_weight = noise(key_list[6], (PROJ, D), HEAD_DIM ** -0.5, 0.5, ((0, 2), (1, 4)))
    cotangent = noise(key_list[7], (TOKENS, D), 0.02, 0.119628906, ((0, 8), (1, 4)))
    return dict(hidden=hidden, neighbour_states=neighbour_states, neighbour_owner=neighbour_owner, query_weight=query_weight, key_weight=key_weight, value_weight=value_weight, out_weight=out_weight, cotangent=cotangent)


def slot_rows(neighbour_owner):
    groups = ALL_SPANS // SPANS_DEV
    flat_owner = neighbour_owner.reshape(groups, SPANS_DEV * NEIGHBOURS).astype(jnp.int32)
    owner_ids = jnp.arange(N_ENC, dtype=jnp.int32)
    onehot = (flat_owner[:, :, None] == owner_ids[None, None, :]).astype(jnp.int32)
    earlier = jnp.cumsum(onehot, axis=1) - onehot
    slot_rank = lax.optimization_barrier(jnp.sum(earlier * onehot, axis=2)).astype(jnp.int32)
    group_base = jnp.arange(groups, dtype=jnp.int32)[:, None] * (N_ENC * SLOTS)
    return (group_base + flat_owner * SLOTS + slot_rank).reshape(ALL_SPANS, NEIGHBOURS).astype(jnp.int32)

def shift_rows(matrix):
    tail_rows = jnp.zeros((SPAN - 1, matrix.shape[1]), matrix.dtype)
    joined = jnp.concatenate([matrix[SPAN - 1:], tail_rows], axis=0)
    return joined.reshape(SPANS_DEV * N_CTX, SPAN, HEADS, HEAD_DIM)

def unshift_rows(blocks):
    flat_rows = blocks.reshape(SPANS_DEV * N_CTX * SPAN, PROJ)
    head_rows = jnp.zeros((SPAN - 1, PROJ), flat_rows.dtype)
    return jnp.concatenate([head_rows, flat_rows[:SEQ_LEN - SPAN + 1]], axis=0)

def attention_grad(cotangent, out_weight):
    width = D // N_ENC
    total = jnp.zeros((SEQ_LEN, PROJ), jnp.float32)
    for block in range(N_ENC):
        cot_cols = cotangent[:, block * width:(block + 1) * width]
        out_cols = out_weight[:, block * width:(block + 1) * width]
        partial_sum = lax.dot_general(cot_cols, out_cols, (((1,), (1,)), ((), ())), preferred_element_type=jnp.float32)
        rounded = lax.optimization_barrier(partial_sum.astype(jnp.bfloat16))
        total = total + rounded.astype(jnp.float32)
    return total.astype(jnp.bfloat16)

def one_sequence(hidden, states, cotangent, query_weight, key_weight, value_weight, out_weight):
    inv_root = 1.0 / math.sqrt(HEAD_DIM)
    span_total = SPANS_DEV * N_CTX
    queries = jnp.dot(hidden, query_weight, preferred_element_type=jnp.float32).astype(jnp.bfloat16)
    flat_states = states.reshape(span_total * NEIGHBOURS * NEIGH_LEN, ENC_D)
    keys = jnp.dot(flat_states, key_weight, preferred_element_type=jnp.float32).astype(jnp.bfloat16)
    values = jnp.dot(flat_states, value_weight, preferred_element_type=jnp.float32).astype(jnp.bfloat16)
    keys = keys.reshape(span_total, NEIGHBOURS * NEIGH_LEN, HEADS, HEAD_DIM).astype(jnp.float32)
    values = values.reshape(span_total, NEIGHBOURS * NEIGH_LEN, HEADS, HEAD_DIM).astype(jnp.float32)
    grouped = shift_rows(queries).astype(jnp.float32)
    scores = jnp.einsum('cqhd,ckhd->chqk', grouped, keys) * inv_root
    probs = jax.nn.softmax(scores, axis=-1)
    rounded = probs.astype(jnp.bfloat16).astype(jnp.float32)
    blocks = jnp.einsum('chqk,ckhd->cqhd', rounded, values)
    attention = unshift_rows(blocks).astype(jnp.bfloat16)
    mixed = jnp.dot(attention, out_weight, preferred_element_type=jnp.float32).astype(jnp.bfloat16)
    grad_attention = attention_grad(cotangent, out_weight)
    grad_grouped = shift_rows(grad_attention).astype(jnp.float32)
    grad_probs = jnp.einsum('cqhd,ckhd->chqk', grad_grouped, values)
    inner = lax.optimization_barrier(jnp.sum(probs * grad_probs, axis=-1, keepdims=True))
    grad_scores = (probs * (grad_probs - inner)).astype(jnp.bfloat16).astype(jnp.float32)
    grad_blocks = jnp.einsum('chqk,ckhd->cqhd', grad_scores, keys) * inv_root
    grad_queries = unshift_rows(grad_blocks).astype(jnp.bfloat16)
    hidden_blocks = hidden.reshape(N_CTX, SPANS_DEV * SPAN, D).astype(jnp.float32)
    grad_blocks_rows = grad_queries.reshape(N_CTX, SPANS_DEV * SPAN, PROJ).astype(jnp.float32)
    parts = jnp.einsum('ntd,ntp->ndp', hidden_blocks, grad_blocks_rows).astype(jnp.bfloat16)
    return (mixed, lax.optimization_barrier(jnp.sum(parts.astype(jnp.float32), axis=0)))

def reference(hidden, neighbour_states, neighbour_owner, query_weight, key_weight, value_weight, out_weight, cotangent):
    rows = slot_rows(neighbour_owner).reshape(N_DP, SPANS_DEV * N_CTX, NEIGHBOURS)
    hidden_seq = hidden.reshape(N_DP, SEQ_LEN, D)
    cotangent_seq = cotangent.reshape(N_DP, SEQ_LEN, D)

    def advance(running, items):
        hidden_one, rows_one, cotangent_one = items
        states = jnp.take(neighbour_states, rows_one.reshape(-1), axis=0)
        mixed_one, grad_one = one_sequence(hidden_one, states, cotangent_one, query_weight, key_weight, value_weight, out_weight)
        return (running + grad_one, mixed_one)
    running, mixed = lax.scan(advance, jnp.zeros((D, PROJ), jnp.float32), (hidden_seq, rows, cotangent_seq))
    return (mixed.reshape(TOKENS, D), running)
```

```python
import functools
import math

import jax
import jax.numpy as jnp
from jax import lax
from jax.experimental import pallas as pl
from jax.experimental.pallas import tpu as pltpu
from jax.sharding import PartitionSpec as P

HEAD_DIM = 128
BF16 = jnp.bfloat16
F32 = jnp.float32


def from_next(value, axis):
    size = lax.axis_size(axis)
    return lax.ppermute(value, axis, [(i, i - 1) for i in range(1, size)])


def from_prev(value, axis):
    size = lax.axis_size(axis)
    return lax.ppermute(value, axis, [(i - 1, i) for i in range(1, size)])


def swap(value, axis, k):
    size = lax.axis_size(axis)
    return lax.ppermute(value, axis, [(i, i ^ k) for i in range(size)])


def spread(value, axis):
    return [value] + [swap(value, axis, k) for k in range(1, lax.axis_size(axis))]


def in_order(parts, axis):
    here = lax.axis_index(axis)
    rows = parts[0].shape[0]
    joined = jnp.zeros((rows * len(parts),) + parts[0].shape[1:], parts[0].dtype)
    for k, part in enumerate(parts):
        joined = lax.dynamic_update_slice_in_dim(joined, part, (here ^ k) * rows, 0)
    return joined


def slot_places(neighbour_owner, owner_count):
    flat_owner = neighbour_owner.reshape(-1)
    owner_ids = jnp.arange(owner_count, dtype=jnp.int32)
    onehot = (flat_owner[:, None] == owner_ids[None, :]).astype(jnp.int32)
    earlier = jnp.cumsum(onehot, axis=0) - onehot
    slot_rank = jnp.sum(earlier * onehot, axis=1)
    return flat_owner, slot_rank


def gather_line(block, axis):
    size = lax.axis_size(axis)
    found = {0: block}
    up = lax.ppermute(block, axis, [(i, i + 1) for i in range(size - 1)])
    down = lax.ppermute(block, axis, [(i + 1, i) for i in range(size - 1)])
    found[-1], found[1] = up, down
    for s in range(2, size):
        found[-s] = lax.ppermute(found[1 - s], axis, [(i, i + 1) for i in range(s - 1, size - 1)])
        found[s] = lax.ppermute(found[s - 1], axis, [(i + 1, i) for i in range(0, size - s)])
    return found


def reduce_line(blocks, axis):
    size = lax.axis_size(axis)
    here = lax.axis_index(axis)
    shape = blocks.shape[1:]

    def ahead(rising, count):
        start = jnp.where(rising, size - count, 0)
        return lax.dynamic_slice_in_dim(blocks, start, count, 0)

    own = lax.dynamic_index_in_dim(blocks, here, 0, keepdims=False).astype(F32)
    carried = None
    for s in range(1, size):
        count = size - s
        rising = here == s - 1
        message = ahead(rising, count)
        if carried is not None:
            rest = jnp.where(rising, carried[1:], carried[:-1])
            message = (message.astype(F32) + rest.astype(F32)).astype(BF16)
        carried_in = lax.ppermute(
            message, axis, [(s - 1, s), (size - s, size - 1 - s)] if size > 1 else []
        )
        from_below = here == s
        arrived = jnp.where(from_below, carried_in[0], carried_in[-1])
        arrives = from_below | (here == size - 1 - s)
        own = own + jnp.where(arrives, arrived.astype(F32), 0.0)
        carried = carried_in
    return own.astype(BF16)


def attend(
    place_ref,
    q_ref,
    ga_ref,
    kw_ref,
    vw_ref,
    *refs,
    source_count,
    per_span,
    head_count,
    span_len,
):
    sources = refs[:source_count]
    main_ref, tail_ref, gq_ref, states, shifted, sems = refs[source_count:]
    step = pl.program_id(0)
    steps = pl.num_programs(0)
    pairs = states.shape[0]
    inv_root = 1.0 / math.sqrt(HEAD_DIM)

    @pl.when(step == 0)
    def _():
        for pair in range(pairs):
            for at in range(source_count):

                @pl.when(place_ref[0, pair] == at)
                def _():
                    pltpu.make_async_copy(
                        sources[at].at[place_ref[1, pair]], states.at[pair], sems.at[pair]
                    ).start()

        shifted[pl.ds(0, span_len), :] = jnp.zeros((span_len, shifted.shape[1]), F32)
        shifted[pl.ds(shifted.shape[0] - span_len, span_len), :] = jnp.zeros(
            (span_len, shifted.shape[1]), F32
        )

    for j in range(per_span):
        pair = step * per_span + j
        pltpu.make_async_copy(sources[0].at[0], states.at[pair], sems.at[pair]).wait()
    rows = states[pl.ds(step * per_span, per_span)]
    rows = rows.reshape(rows.shape[0] * rows.shape[1], rows.shape[2])
    keys = jnp.dot(rows, kw_ref[...], preferred_element_type=F32).astype(BF16)
    values = jnp.dot(rows, vw_ref[...], preferred_element_type=F32).astype(BF16)
    nt = (((1,), (1,)), ((), ()))
    outs = []
    for h in range(head_count):
        cols = slice(h * HEAD_DIM, (h + 1) * HEAD_DIM)
        key, value = keys[:, cols], values[:, cols]
        q = q_ref[:, cols]
        ga = ga_ref[:, cols]
        scores = lax.dot_general(q, key, nt, preferred_element_type=F32) * inv_root
        top = jnp.max(scores, axis=-1, keepdims=True)
        raised = jnp.exp(scores - top)
        probs = raised / jnp.sum(raised, axis=-1, keepdims=True)
        outs.append(jnp.dot(probs.astype(BF16), value, preferred_element_type=F32))
        grad_probs = lax.dot_general(ga, value, nt, preferred_element_type=F32)
        inner = jnp.sum(probs * grad_probs, axis=-1, keepdims=True)
        grad_scores = (probs * (grad_probs - inner)).astype(BF16)
        gq = jnp.dot(grad_scores, key, preferred_element_type=F32) * inv_root
        gq_ref[:, cols] = gq.astype(BF16)
    for c in range(main_ref.shape[0] // span_len):

        @pl.when(step == c)
        def _():
            for h in range(head_count):
                shifted[
                    pl.ds(span_len - 1 + c * span_len, span_len),
                    h * HEAD_DIM : (h + 1) * HEAD_DIM,
                ] = outs[h]

    @pl.when(step == steps - 1)
    def _():
        size = main_ref.shape[0]
        main_ref[...] = shifted[pl.ds(0, size), :].astype(BF16)
        tail_ref[...] = shifted[pl.ds(size, span_len), :].astype(BF16)


def attention(place, queries, grad_attention, key_full, value_full, sources, span_count):
    tok_rows, width = queries.shape
    span_len = tok_rows // span_count
    pairs = place.shape[1]
    head_count = width // HEAD_DIM
    _, length, enc_width = sources[0].shape
    body = functools.partial(
        attend,
        source_count=len(sources),
        per_span=pairs // span_count,
        head_count=head_count,
        span_len=span_len,
    )
    rows = pl.BlockSpec((span_len, width), lambda c: (c, 0))
    whole = pl.BlockSpec((enc_width, width), lambda c: (0, 0))
    return pl.pallas_call(
        body,
        grid=(span_count,),
        in_specs=[pl.BlockSpec(memory_space=pltpu.SMEM), rows, rows, whole, whole]
        + [pl.BlockSpec(memory_space=pl.ANY)] * len(sources),
        out_specs=[
            pl.BlockSpec((tok_rows, width), lambda c: (0, 0)),
            pl.BlockSpec((span_len, width), lambda c: (0, 0)),
            rows,
        ],
        out_shape=[
            jax.ShapeDtypeStruct((tok_rows, width), BF16),
            jax.ShapeDtypeStruct((span_len, width), BF16),
            jax.ShapeDtypeStruct((tok_rows, width), BF16),
        ],
        scratch_shapes=[
            pltpu.VMEM((pairs, length, enc_width), BF16),
            pltpu.VMEM((tok_rows + span_len, width), F32),
            pltpu.SemaphoreType.DMA((pairs,)),
        ],
        compiler_params=pltpu.CompilerParams(dimension_semantics=("arbitrary",)),
        name="attend",
    )(place, queries, grad_attention, key_full, value_full, *sources)


def shards(
    hidden,
    neighbour_states,
    neighbour_owner,
    query_weight,
    key_weight,
    value_weight,
    out_weight,
    cotangent,
):
    dp_count = lax.axis_size("dp")
    ctx_count = lax.axis_size("ctx")
    enc_count = lax.axis_size("enc")
    dp_at, ctx_at, enc_at = (lax.axis_index(axis) for axis in ("dp", "ctx", "enc"))
    span_count = neighbour_owner.shape[0]
    tok_rows, model_width = hidden.shape
    span_len = tok_rows // span_count
    local_proj = query_weight.shape[1]
    share = model_width // (dp_count * ctx_count)

    found = gather_line(neighbour_states, "enc")
    distances = list(found)
    flat_owner, slot_rank = slot_places(neighbour_owner, enc_count)
    away = flat_owner - enc_at
    place = jnp.stack(
        [sum(jnp.where(away == d, at, 0) for at, d in enumerate(distances)), slot_rank]
    ).astype(jnp.int32)

    def shift(matrix):
        ahead = from_next(matrix[:span_len], "ctx")
        return jnp.concatenate([matrix[span_len - 1 :], ahead[: span_len - 1]], axis=0)

    hidden_shifted = shift(hidden)
    cotangent_shifted = shift(cotangent)

    out_full = in_order(spread(out_weight, "dp"), "dp")
    key_full = in_order(spread(key_weight, "dp"), "dp")
    value_full = in_order(spread(value_weight, "dp"), "dp")
    query_full = in_order(spread(query_weight, "dp"), "dp")

    grad_partial = [
        lax.dot_general(
            cotangent_shifted,
            out_full[e * local_proj : (e + 1) * local_proj],
            (((1,), (1,)), ((), ())),
            preferred_element_type=F32,
        ).astype(BF16)
        for e in range(enc_count)
    ]
    grad_attention = reduce_line(jnp.stack(grad_partial), "enc")
    queries = jnp.dot(hidden_shifted, query_full, preferred_element_type=F32).astype(BF16)

    def columns(d, c):
        return lax.dynamic_slice_in_dim(
            hidden_shifted, d * (share * ctx_count) + c * share, share, 1
        )

    by_ctx = []
    for k in range(ctx_count):
        block = jnp.concatenate([columns(dp_at ^ j, ctx_at ^ k) for j in range(dp_count)], axis=0)
        by_ctx.append(swap(block, "ctx", k) if k else block)
    hidden_share = []
    for j in range(dp_count):
        block = jnp.concatenate([b[j * tok_rows : (j + 1) * tok_rows] for b in by_ctx], axis=0)
        hidden_share.append(swap(block, "dp", j) if j else block)
    hidden_share = jnp.concatenate(hidden_share, axis=0)

    main, tail, grad_queries = attention(
        place,
        queries,
        grad_attention,
        key_full,
        value_full,
        [found[d] for d in distances],
        span_count,
    )

    grads = jnp.concatenate(spread(grad_queries, "ctx"), axis=0)
    grads = jnp.concatenate(spread(grads, "dp"), axis=0)
    grad_share = lax.dot_general(
        hidden_share, grads, (((0,), (0,)), ((), ())), preferred_element_type=F32
    ).astype(BF16)
    parts = spread(grad_share, "ctx")
    grad_query = in_order([part.astype(F32) for part in parts], "ctx")

    before = from_prev(tail, "ctx")
    attended = jnp.concatenate([main[:span_len] + before, main[span_len:]], axis=0)
    mixed = 0.0
    for k, part in enumerate(spread(attended, "enc")):
        rows = lax.dynamic_slice_in_dim(out_full, (enc_at ^ k) * local_proj, local_proj, 0)
        mixed = mixed + jnp.dot(part, rows, preferred_element_type=F32)
    return mixed.astype(BF16), grad_query


def solution(mesh):
    placed = (
        P(("dp", "ctx"), None),
        P(("dp", "ctx", "enc"), None, None),
        P(("dp", "ctx"), None),
        P("dp", "enc"),
        P("dp", "enc"),
        P("dp", "enc"),
        P("dp", "enc"),
        P(("dp", "ctx"), "enc"),
    )
    return jax.shard_map(
        shards,
        mesh=mesh,
        in_specs=placed,
        out_specs=(P(("dp", "ctx"), "enc"), P("dp", "enc")),
        check_vma=False,
    )
```

```python
import functools
import math

import jax
import jax.numpy as jnp
from jax import lax
from jax.experimental import pallas as pl
from jax.experimental.pallas import tpu as pltpu
from jax.sharding import PartitionSpec as P


HEAD_DIM = 128
BF16 = jnp.bfloat16
F32 = jnp.float32


def from_next(value, axis):
    size = lax.axis_size(axis)
    return lax.ppermute(value, axis, [(i, i - 1) for i in range(1, size)])


def from_prev(value, axis):
    size = lax.axis_size(axis)
    return lax.ppermute(value, axis, [(i - 1, i) for i in range(1, size)])


def swap(value, axis, k):
    size = lax.axis_size(axis)
    return lax.ppermute(value, axis, [(i, i ^ k) for i in range(size)])


def spread(value, axis):
    return [value] + [swap(value, axis, k) for k in range(1, lax.axis_size(axis))]


def in_order(parts, axis, dim=0):
    here = lax.axis_index(axis)
    size = parts[0].shape[dim]
    shape = list(parts[0].shape)
    shape[dim] = size * len(parts)
    joined = jnp.zeros(shape, parts[0].dtype)
    for k, part in enumerate(parts):
        joined = lax.dynamic_update_slice_in_dim(joined, part, (here ^ k) * size, dim)
    return joined


def slot_places(neighbour_owner, owner_count):
    flat_owner = neighbour_owner.reshape(-1)
    owner_ids = jnp.arange(owner_count, dtype=jnp.int32)
    onehot = (flat_owner[:, None] == owner_ids[None, :]).astype(jnp.int32)
    earlier = jnp.cumsum(onehot, axis=0) - onehot
    slot_rank = jnp.sum(earlier * onehot, axis=1)
    return flat_owner, slot_rank


def gather_line(block, axis):
    size = lax.axis_size(axis)
    found = {0: block}
    for s in range(1, size):
        found[-s] = lax.ppermute(found[1 - s], axis, [(i, i + 1) for i in range(s - 1, size - 1)])
        found[s] = lax.ppermute(
            found[s - 1], axis, [(i + 1, i) for i in range(0, size - s)]
        )
    return found


def reduce_line(partial, axis):
    size = lax.axis_size(axis)
    here = lax.axis_index(axis)
    width = partial.shape[1] // size

    def columns(matrix, at, count):
        return lax.dynamic_slice_in_dim(matrix, at * width, count * width, 1)

    own = columns(partial, here, 1).astype(F32)
    carried = None
    for s in range(1, size):
        count = size - s
        rising = here == s - 1
        message = columns(partial, jnp.where(rising, s, 0), count)
        if carried is not None:
            rest = columns(carried, jnp.where(rising, 1, 0), count)
            message = (message.astype(F32) + rest.astype(F32)).astype(BF16)
        carried = lax.ppermute(message, axis, [(s - 1, s), (size - s, size - 1 - s)])
        arrived = columns(carried, jnp.where(here == s, 0, count - 1), 1)
        arrives = (here == s) | (here == size - 1 - s)
        own = own + jnp.where(arrives, arrived.astype(F32), 0.0)
    return own.astype(BF16)


def turn(at_ref, own_ref, ahead_ref, rows_ref, *refs, ctx_count, dp_count):
    messages, (joined, turned, sems) = refs[:-3], refs[-3:]
    size, first = own_ref.shape[0], ahead_ref.shape[0] - 1
    share = own_ref.shape[1]
    half = share // 2
    joined[pl.ds(0, size), :] = own_ref[...].astype(F32)
    joined[pl.ds(size, first + 1), :] = ahead_ref[...].astype(F32)
    rows = joined[pl.ds(first, size), :].astype(BF16)
    rows_ref[...] = rows
    step = pl.program_id(0)
    eye = lax.broadcasted_iota(jnp.int32, (share, share), 0) == lax.broadcasted_iota(
        jnp.int32, (share, share), 1
    )
    turned[step] = lax.dot_general(
        eye.astype(F32).astype(BF16), rows, (((1,), (1,)), ((), ())), preferred_element_type=F32
    ).astype(BF16)

    def copies(at):
        j, m = divmod(at, ctx_count)
        targets = [(m, 0, 1), (m ^ 2, 1, 1), (m, 2, 0), (m ^ 1, 3, 0)]
        out = []
        for i, (k, place, upper) in enumerate(targets):
            if k:
                target = messages[dp_count - 1 + k].at[j, place]
            else:
                target = messages[j].at[place]
            source = turned.at[at, pl.ds(upper * half, half)]
            out.append(pltpu.make_async_copy(source, target, sems.at[at, i]))
        return out

    steps = ctx_count * dp_count
    for at in range(steps):

        @pl.when(step == at)
        def _():
            for copy in copies(at):
                copy.start()

    @pl.when(step == steps - 1)
    def _():
        for at in range(steps):
            for copy in copies(at):
                copy.wait()


def shift_and_turn_plain(matrix, ahead, dp_at, ctx_at, dp_count, ctx_count):
    first = ahead.shape[0] - 1
    rows = jnp.concatenate([matrix[first:], ahead[:first]], axis=0)
    size = rows.shape[1] // dp_count
    share = size // ctx_count
    half = share // 2
    shifted, own, away = [], [], [[] for _ in range(ctx_count - 1)]
    for j in range(dp_count):
        columns = lax.dynamic_slice_in_dim(rows, (dp_at ^ j) * size, size, 1)
        shifted.append(columns)
        turned = columns.T
        for k in range(ctx_count):
            peer = ctx_at ^ k
            places = [(peer, 1), (peer ^ 2, 1), (peer, 0), (peer ^ 1, 0)]
            block = jnp.stack(
                [
                    lax.dynamic_slice_in_dim(turned, q * share + upper * half, half, 0)
                    for q, upper in places
                ]
            )
            (away[k - 1] if k else own).append(block)
    return jnp.concatenate(shifted, axis=1), own, [jnp.stack(blocks) for blocks in away]


def shift_and_turn(matrix, ahead, dp_at, ctx_at, dp_count, ctx_count):
    rows, width = matrix.shape
    share = width // (dp_count * ctx_count)
    if share % 128:
        return shift_and_turn_plain(matrix, ahead, dp_at, ctx_at, dp_count, ctx_count)

    def source(i, at):
        return (i // ctx_count ^ at[0]) * ctx_count + (i % ctx_count ^ at[1])

    def target(i, at):
        return (i // ctx_count) * ctx_count + (i % ctx_count ^ at[1])

    own = jax.ShapeDtypeStruct((4, share // 2, rows), BF16)
    away = jax.ShapeDtypeStruct((dp_count, 4, share // 2, rows), BF16)
    outs = [own] * dp_count + [away] * (ctx_count - 1)
    shifted, *messages = pl.pallas_call(
        functools.partial(turn, ctx_count=ctx_count, dp_count=dp_count),
        grid_spec=pltpu.PrefetchScalarGridSpec(
            num_scalar_prefetch=1,
            grid=(dp_count * ctx_count,),
            in_specs=[
                pl.BlockSpec((rows, share), lambda i, at: (0, source(i, at))),
                pl.BlockSpec((ahead.shape[0], share), lambda i, at: (0, source(i, at))),
            ],
            out_specs=[pl.BlockSpec((rows, share), lambda i, at: (0, target(i, at)))]
            + [pl.BlockSpec(memory_space=pl.ANY)] * len(outs),
            scratch_shapes=[
                pltpu.VMEM((rows + ahead.shape[0], share), F32),
                pltpu.VMEM((dp_count * ctx_count, share, rows), BF16),
                pltpu.SemaphoreType.DMA((dp_count * ctx_count, 4)),
            ],
        ),
        out_shape=[jax.ShapeDtypeStruct((rows, width), BF16)] + outs,
        compiler_params=pltpu.CompilerParams(dimension_semantics=("arbitrary",)),
        name="turn",
    )(jnp.stack([dp_at, ctx_at]).astype(jnp.int32), matrix, ahead)
    return shifted, messages[:dp_count], messages[dp_count:]


def attend(
    place_ref,
    q_ref,
    ga_ref,
    *refs,
    source_count,
    part_count,
    per_span,
    head_count,
    span_len,
):
    sources, refs = refs[:source_count], refs[source_count:]
    parts, refs = refs[: 2 * part_count], refs[2 * part_count :]
    main_ref, tail_ref, gq_ref, states, weights, raw, sems, part_sems = refs
    step = pl.program_id(0)
    steps = pl.num_programs(0)
    pairs = states.shape[0]
    width = raw.shape[1]
    inv_root = 1.0 / math.sqrt(HEAD_DIM)

    copies = [
        pltpu.make_async_copy(
            part,
            weights.at[
                i // part_count,
                pl.ds(pl.multiple_of(place_ref[2, i % part_count], 16), part.shape[0]),
            ],
            part_sems.at[i],
        )
        for i, part in enumerate(parts)
    ]

    @pl.when(step == 0)
    def _():
        for copy in copies:
            copy.start()
        for pair in range(pairs):
            for at in range(source_count):

                @pl.when(place_ref[0, pair] == at)
                def _():
                    pltpu.make_async_copy(
                        sources[at].at[place_ref[1, pair]], states.at[pair], sems.at[pair]
                    ).start()

        raw[pl.ds(0, span_len), :] = jnp.zeros((span_len, width), F32)
        raw[pl.ds(raw.shape[0] - 8, 8), :] = jnp.zeros((8, width), F32)

    @pl.when(step == 0)
    def _():
        for copy in copies:
            copy.wait()

    for j in range(per_span):
        pair = step * per_span + j
        pltpu.make_async_copy(sources[0].at[0], states.at[pair], sems.at[pair]).wait()
    rows = states[pl.ds(step * per_span, per_span)]
    rows = rows.reshape(rows.shape[0] * rows.shape[1], rows.shape[2])
    keys = jnp.dot(rows, weights[0], preferred_element_type=F32).astype(BF16)
    values = jnp.dot(rows, weights[1], preferred_element_type=F32).astype(BF16)
    nt = (((1,), (1,)), ((), ()))

    def split(x):
        return [x[:, h * HEAD_DIM : (h + 1) * HEAD_DIM] for h in range(head_count)]

    keys, values, q, ga = split(keys), split(values), split(q_ref[...]), split(ga_ref[...])
    scores = [
        lax.dot_general(a, b, nt, preferred_element_type=F32) * inv_root for a, b in zip(q, keys)
    ]
    grad_probs = [
        lax.dot_general(a, b, nt, preferred_element_type=F32) for a, b in zip(ga, values)
    ]
    top = [jnp.max(x, axis=-1, keepdims=True) for x in scores]
    raised = [jnp.exp(x - t) for x, t in zip(scores, top)]
    total = [jnp.sum(x, axis=-1, keepdims=True) for x in raised]
    probs = [x / t for x, t in zip(raised, total)]
    outs = [
        jnp.dot(p.astype(BF16), v, preferred_element_type=F32) for p, v in zip(probs, values)
    ]
    inner = [jnp.sum(p * g, axis=-1, keepdims=True) for p, g in zip(probs, grad_probs)]
    grad_scores = [
        (p * (g - i)).astype(BF16) for p, g, i in zip(probs, grad_probs, inner)
    ]
    gq = [
        jnp.dot(g, k, preferred_element_type=F32) * inv_root for g, k in zip(grad_scores, keys)
    ]
    gq_ref[...] = jnp.concatenate(gq, axis=1).astype(BF16)
    at = pl.multiple_of((step + 1) * span_len, span_len)
    raw[pl.ds(at, span_len), :] = jnp.concatenate(outs, axis=1)

    @pl.when(step == steps - 1)
    def _():
        size = main_ref.shape[0]
        main_ref[...] = raw[pl.ds(1, size), :].astype(BF16)
        tail_ref[...] = raw[pl.ds(size + 1, span_len), :].astype(BF16)


def attention(place, queries, grad_attention, key_parts, value_parts, sources, span_count):
    tok_rows, width = queries.shape
    span_len = tok_rows // span_count
    pairs = place.shape[1]
    head_count = width // HEAD_DIM
    _, length, enc_width = sources[0].shape
    body = functools.partial(
        attend,
        source_count=len(sources),
        part_count=len(key_parts),
        per_span=pairs // span_count,
        head_count=head_count,
        span_len=span_len,
    )
    rows = pl.BlockSpec((span_len, width), lambda c: (c, 0))
    return pl.pallas_call(
        body,
        grid=(span_count,),
        in_specs=[pl.BlockSpec(memory_space=pltpu.SMEM), rows, rows]
        + [pl.BlockSpec(memory_space=pl.ANY)] * (len(sources) + 2 * len(key_parts)),
        out_specs=[
            pl.BlockSpec((tok_rows, width), lambda c: (0, 0)),
            pl.BlockSpec((span_len, width), lambda c: (0, 0)),
            rows,
        ],
        out_shape=[
            jax.ShapeDtypeStruct((tok_rows, width), BF16),
            jax.ShapeDtypeStruct((span_len, width), BF16),
            jax.ShapeDtypeStruct((tok_rows, width), BF16),
        ],
        scratch_shapes=[
            pltpu.VMEM((pairs, length, enc_width), BF16),
            pltpu.VMEM((2, enc_width, width), BF16),
            pltpu.VMEM((tok_rows + span_len + 8, width), F32),
            pltpu.SemaphoreType.DMA((pairs,)),
            pltpu.SemaphoreType.DMA((2 * len(key_parts),)),
        ],
        compiler_params=pltpu.CompilerParams(dimension_semantics=("arbitrary",)),
        name="attend",
    )(place, queries, grad_attention, *sources, *key_parts, *value_parts)


def share_grad(*refs, block_count):
    upper_ref, lower_ref = refs[-2:]
    count = (len(refs) - 2) // 2
    feats, grads = refs[:count], refs[count:-2]
    total = None
    for j in range(0, count, block_count):
        sums = [
            jnp.dot(
                feats[i][...].reshape(feats[i].shape[-2:]),
                grads[i][...],
                preferred_element_type=F32,
            )
            for i in range(j, j + block_count)
        ]
        while len(sums) > 1:
            sums = [sums[i] + sums[i + 1] for i in range(0, len(sums), 2)]
        total = sums[0] if total is None else total + sums[0]
    step = pl.program_id(0)

    @pl.when(step < 2)
    def _():
        upper_ref[step] = total.astype(BF16)

    @pl.when(step >= 2)
    def _():
        lower_ref[step - 2] = total.astype(BF16)


def weight_share(features, grads, block_count):
    parts, rows, tokens = features[0].shape[-3:]
    width = grads[0].shape[1]
    specs = [
        pl.BlockSpec((1, rows, tokens), lambda i: (i, 0, 0))
        if x.ndim == 3
        else pl.BlockSpec((1, 1, rows, tokens), lambda i: (0, i, 0, 0))
        for x in features
    ]
    return pl.pallas_call(
        functools.partial(share_grad, block_count=block_count),
        grid=(parts,),
        in_specs=specs + [pl.BlockSpec((tokens, width), lambda i: (0, 0))] * len(grads),
        out_specs=[pl.BlockSpec((2, rows, width), lambda i: (0, 0, 0))] * 2,
        out_shape=[jax.ShapeDtypeStruct((2, rows, width), BF16)] * 2,
        compiler_params=pltpu.CompilerParams(dimension_semantics=("arbitrary",)),
        name="weight_share",
    )(*features, *grads)


def place_rows(order_ref, *refs, picks):
    *sources, out_ref = refs
    for step, (source, row) in enumerate(picks):

        @pl.when(pl.program_id(0) == step)
        def _():
            out_ref[...] = sources[source][row].astype(F32)


def assemble(order, sources, picks, base=None):
    _, rows, width = sources[0].shape
    count = 4 * len(sources)
    specs = [pl.BlockSpec(x.shape, lambda i, order: (0, 0, 0)) for x in sources]
    held = []
    body = functools.partial(place_rows, picks=picks)
    if base is not None:
        specs, held = [pl.BlockSpec(memory_space=pl.ANY)] + specs, [base]
        inner = body
        body = lambda order_ref, base_ref, *refs: inner(order_ref, *refs)
    return pl.pallas_call(
        body,
        grid_spec=pltpu.PrefetchScalarGridSpec(
            num_scalar_prefetch=1,
            grid=(len(picks),),
            in_specs=specs,
            out_specs=pl.BlockSpec((rows, width), lambda i, order: (order[i], 0)),
        ),
        out_shape=jax.ShapeDtypeStruct((count * rows, width), F32),
        input_output_aliases={1: 0} if held else {},
        compiler_params=pltpu.CompilerParams(dimension_semantics=("arbitrary",)),
        name="assemble",
    )(order, *held, *sources)


def shards(
    hidden,
    neighbour_states,
    neighbour_owner,
    query_weight,
    key_weight,
    value_weight,
    out_weight,
    cotangent,
):
    dp_count = lax.axis_size("dp")
    ctx_count = lax.axis_size("ctx")
    enc_count = lax.axis_size("enc")
    dp_at, ctx_at, enc_at = (lax.axis_index(axis) for axis in ("dp", "ctx", "enc"))
    span_count = neighbour_owner.shape[0]
    tok_rows, _ = hidden.shape
    span_len = tok_rows // span_count
    local_proj = query_weight.shape[1]

    found = gather_line(neighbour_states, "enc")
    distances = list(found)

    hidden_ahead = from_next(hidden[:span_len], "ctx")
    cotangent_ahead = from_next(cotangent[:span_len], "ctx")
    cotangent_shifted = jnp.concatenate(
        [cotangent[span_len - 1 :], cotangent_ahead[: span_len - 1]], axis=0
    )
    out_parts = spread(out_weight, "dp")
    query_parts = spread(query_weight, "dp")
    key_parts, value_parts = spread(key_weight, "dp"), spread(value_weight, "dp")
    hidden_shifted, own_features, away_features = shift_and_turn(
        hidden, hidden_ahead, dp_at, ctx_at, dp_count, ctx_count
    )
    features = [own_features[0]]
    for k in range(1, ctx_count):
        features.append(swap(away_features[k - 1], "ctx", k))
    for j in range(1, dp_count):
        for k in range(ctx_count):
            features.append(swap(features[k][j] if k else own_features[j], "dp", j))

    partials = []
    for part in out_parts:
        partials.append(
            lax.dot_general(
                cotangent_shifted,
                part,
                (((1,), (1,)), ((), ())),
                preferred_element_type=F32,
            ).astype(BF16)
        )
    grad_attention = reduce_line(in_order(partials, "dp", 1), "enc")

    queries = 0.0
    for j, part in enumerate(query_parts):
        size = part.shape[0]
        queries = queries + jnp.dot(
            hidden_shifted[:, j * size : (j + 1) * size], part, preferred_element_type=F32
        )
    queries = queries.astype(BF16)

    flat_owner, slot_rank = slot_places(neighbour_owner, enc_count)
    away = flat_owner - enc_at
    source = sum(jnp.where(away == d, at, 0) for at, d in enumerate(distances))
    if key_weight.shape[0] % 16:
        key_parts = [in_order(key_parts, "dp")]
        value_parts = [in_order(value_parts, "dp")]
        starts = jnp.zeros_like(source)
    else:
        starts = (dp_at ^ jnp.arange(source.shape[0])) * key_weight.shape[0]
    place = jnp.stack([source, slot_rank, starts]).astype(jnp.int32)
    out_full = in_order(out_parts, "dp")

    main, tail, grad_queries = attention(
        place,
        queries,
        grad_attention,
        key_parts,
        value_parts,
        [found[d] for d in distances],
        span_count,
    )

    before = from_prev(tail, "ctx")
    attended = jnp.concatenate([main[:span_len] + before, main[span_len:]], axis=0)
    mixed = 0.0
    for k in range(enc_count):
        part = swap(attended, "enc", k) if k else attended
        rows = lax.dynamic_slice_in_dim(out_full, (enc_at ^ k) * local_proj, local_proj, 0)
        mixed = mixed + jnp.dot(part, rows, preferred_element_type=F32)

    grads = []
    for k in range(ctx_count):
        grads.append(swap(grad_queries, "ctx", k) if k else grad_queries)
    for j in range(1, dp_count):
        for k in range(ctx_count):
            grads.append(swap(grads[k], "dp", j))
    uppers, lowers = weight_share(features, grads, ctx_count)
    uppers_in = swap(uppers, "ctx", 1)
    lowers_in = swap(lowers, "ctx", 2)

    def put(picks, sources, base=None):
        order = jnp.stack([(ctx_at ^ k) * 2 + upper for k, upper, _, _ in picks])
        return assemble(
            order.astype(jnp.int32), sources, tuple((a, r) for _, _, a, r in picks), base
        )

    grad_query = put([(0, 0, 1, 0), (0, 1, 0, 0), (1, 0, 1, 1), (2, 1, 0, 1)], [uppers, lowers])
    grad_query = put(
        [(1, 1, 0, 0), (3, 1, 0, 1), (2, 0, 1, 0), (3, 0, 1, 1)],
        [uppers_in, lowers_in],
        grad_query,
    )
    return mixed.astype(BF16), grad_query


def solution(mesh):
    placed = (
        P(("dp", "ctx"), None),
        P(("dp", "ctx", "enc"), None, None),
        P(("dp", "ctx"), None),
        P("dp", "enc"),
        P("dp", "enc"),
        P("dp", "enc"),
        P("dp", "enc"),
        P(("dp", "ctx"), "enc"),
    )

    return jax.shard_map(
        shards,
        mesh=mesh,
        in_specs=placed,
        out_specs=(P(("dp", "ctx"), "enc"), P("dp", "enc")),
        check_vma=False,
    )
```
